32 devices in a mesh: gx: 4 (over y, x), gy: 4 (over z), gz: 2 (over core).
Axes of the slice: x: 2, y: 2, z: 4, core: 2. Of those that a mesh axis runs over, the one named last changes fastest.
Arguments:
- right_side: float32 [5, 512, 8, 128], P(None, ('gx', 'gy', 'gz')), may hold values from -6 to 6
- diag_inverse: bfloat16 [5, 512, 128, 128], P(None, ('gx', 'gy', 'gz')), may hold values from -0.5 to 0.5
- off_blocks: bfloat16 [4, 1024, 128, 128], P(None, ('gx', 'gy', 'gz')), may hold values from -0.375 to 0.375
- live_counts: int32 [5, 32], P(None, ('gx', 'gy', 'gz')), may hold values from 1 to 16, as said below
- source_slot: int32 [4, 1024], P(None, ('gx', 'gy', 'gz')), may hold values from 0 to 15, as said below
- target_owner: int32 [4, 1024], P(None, ('gx', 'gy', 'gz')), may hold values from 0 to 31, as said below
- target_block: int32 [4, 1024], P(None, ('gx', 'gy', 'gz')), may hold values from 16 to 79, as said below
Outputs:
- solution: float32 [5, 512, 8, 128], P(None, ('gx', 'gy', 'gz'))
The draws below stay inside these ranges and needn't reach their ends.
Inputs may be any that keep to these rules, and one draw needn't show every extreme that they name: `live_counts`: slots at or past a device's count in a level are empty; in every level some device has all 16 slots live. `source_slot`: names a live slot of the issuing device in the same level. `target_owner`: in every level, each device's records go exactly 2 each to 16 distinct owners and none to the others. `target_block`: the level part is later than the record's own level, and the slot is live at the owner in that level.
All inputs are finite; a program needn't handle non-finite values.
Results may differ from the reference program's by a relative error of at most 0.013.
Values sent between devices are 32-bit elements; how exact they have to be, the bound alone decides.
A program may use at most 64 MiB of HBM per device.

```python
import jax
import jax.numpy as jnp
from jax import lax

B = 128
R = 8
LEVELS = 5
S = 16
CAP = 2
OWNERS = 32
RECS = 32
NBLK = 512


def routing(key):
    base = jax.random.fold_in(key, 7)
    key_count, key_full, key_perm, key_src, key_level, key_slot = jax.random.split(base, 6)
    counts = jax.random.randint(key_count, (LEVELS, OWNERS), 1, S + 1)
    full_owner = jax.random.randint(key_full, (LEVELS,), 0, OWNERS)
    counts = counts.at[jnp.arange(LEVELS), full_owner].set(S)

    def one_list(sub_key):
        first_key, second_key = jax.random.split(sub_key)
        chosen = jax.random.permutation(first_key, OWNERS)[:OWNERS // 2].astype(jnp.int32)
        whole_list = jnp.repeat(chosen, CAP)
        return whole_list[jax.random.permutation(second_key, RECS)]
    list_keys = jax.random.split(key_perm, (LEVELS - 1) * OWNERS)
    owners = jax.vmap(one_list)(list_keys).reshape(LEVELS - 1, OWNERS, RECS)
    shape = (LEVELS - 1, OWNERS, RECS)
    sources = jax.random.randint(key_src, shape, 0, counts[:-1, :, None])
    lowest = (jnp.arange(LEVELS - 1, dtype=jnp.int32) + 1)[:, None, None]
    target_level = jax.random.randint(key_level, shape, lowest, LEVELS)
    target_slot = jax.random.randint(key_slot, shape, 0, counts[target_level, owners])
    blocks = target_level * S + target_slot
    flat = (LEVELS - 1, OWNERS * RECS)
    return (counts.astype(jnp.int32), sources.reshape(flat).astype(jnp.int32), owners.reshape(flat).astype(jnp.int32), blocks.reshape(flat).astype(jnp.int32))


def draw_live_counts(key, part):
    return routing(key)[0]


def draw_source_slot(key, part):
    return routing(key)[1]


def draw_target_owner(key, part):
    return routing(key)[2]


def draw_target_block(key, part):
    return routing(key)[3]


def block_scale(stream_key, shape, cuts, low, high):
    def one(position, shards_of):
        steps = jax.random.uniform(jax.random.fold_in(jax.random.fold_in(stream_key, 6), position), (shards_of,), jnp.float32, low / len(cuts), high / len(cuts))
        return jnp.repeat(jnp.exp(steps), shape[position] // shards_of).reshape((-1,) + (1,) * (len(shape) - position - 1))

    gain = one(*cuts[0])
    for cut in cuts[1:]:
        gain = gain * one(*cut)
    return gain


def scatter_about(own_key, shape, scale, bound, cuts=(), kind=jnp.bfloat16):
    drawn = scale * jax.random.normal(own_key, shape, jnp.float32)
    if cuts:
        drawn = drawn * block_scale(own_key, shape, cuts, -0.22, 0.18)
    return jnp.clip(drawn, -bound, bound).astype(kind)


def setup_inputs(seed: int = 0) -> dict:
    streams_of = jax.random.split(jax.random.key(seed), 8)
    right_side = scatter_about(streams_of[0], (LEVELS, NBLK, R, B), 1.0, 6.0, ((1, 32),), jnp.float32)
    diag_inverse = scatter_about(streams_of[1], (LEVELS, NBLK, B, B), B ** -0.5, 0.5, ((1, 32),))
    off_blocks = scatter_about(streams_of[2], (LEVELS - 1, OWNERS * RECS, B, B), (2 * B) ** -0.5, 0.375, ((1, 32),))
    live_counts = draw_live_counts(jax.random.fold_in(streams_of[7], 71), 0)
    source_slot = draw_source_slot(jax.random.fold_in(streams_of[7], 71), 0)
    target_owner = draw_target_owner(jax.random.fold_in(streams_of[7], 71), 0)
    target_block = draw_target_block(jax.random.fold_in(streams_of[7], 71), 0)
    return {"right_side": right_side, "diag_inverse": diag_inverse, "off_blocks": off_blocks, "live_counts": live_counts, "source_slot": source_slot, "target_owner": target_owner, "target_block": target_block}


def reference(right_side, diag_inverse, off_blocks, live_counts, source_slot, target_owner, target_block):
    accumulated = jnp.zeros((LEVELS * NBLK, R, B), jnp.float32)
    slot_ids = jnp.arange(S, dtype=jnp.int32)
    solved_all = []
    for level_at in range(LEVELS):
        live = (slot_ids[None, :] < live_counts[level_at][:, None]).reshape(NBLK)
        pending = accumulated[level_at * NBLK:(level_at + 1) * NBLK]
        work_rows = (right_side[level_at] - pending).astype(jnp.bfloat16)
        solved = jnp.einsum('nrb,nbc->nrc', work_rows.astype(jnp.float32), diag_inverse[level_at].astype(jnp.float32))
        solved = jnp.where(live[:, None, None], solved, jnp.float32(0.0))
        solved_all.append(solved)
        if level_at + 1 < LEVELS:
            rounded = solved.astype(jnp.bfloat16).reshape(OWNERS, S, R, B)
            blocks = off_blocks[level_at].reshape(OWNERS, RECS, B, B)
            slot_lists = source_slot[level_at].reshape(OWNERS, RECS)

            def per_owner(items):
                owner_rows, owner_blocks, owner_slots = items
                picked = owner_rows[owner_slots]
                return jnp.einsum('krb,kbc->krc', picked.astype(jnp.float32), owner_blocks.astype(jnp.float32))

            contributions = lax.map(per_owner, (rounded, blocks, slot_lists)).reshape(OWNERS * RECS, R, B)
            owner_ids = target_owner[level_at].astype(jnp.int32)
            targets = target_block[level_at].astype(jnp.int32)
            row_ids = (targets // S) * NBLK + owner_ids * S + targets % S
            accumulated = accumulated.at[row_ids].add(contributions)
    return jnp.stack(solved_all)
```

```python
import functools

import jax
import jax.numpy as jnp
from jax import lax
from jax.experimental import pallas as pl
from jax.experimental.pallas import tpu as pltpu
from jax.sharding import PartitionSpec as P

CAP = 2
GROUPS = 4
CHUNK = 32
TILE = 8
AXES = ("gx", "gy", "gz")
MESH = pl.DeviceIdType.MESH


def kernel(
    sizes,
    live_hbm,
    source_hbm,
    owner_hbm,
    block_hbm,
    right_hbm,
    diag_hbm,
    off_hbm,
    out_ref,
    live_ref,
    source_ref,
    owner_ref,
    block_ref,
    right_ref,
    work_ref,
    diag_ref,
    off_refs,
    solved_ref,
    made_ref,
    outgoing_ref,
    arrived_ref,
    placer_ref,
    names_out_ref,
    names_ref,
    record_vmem,
    record_ref,
    small_sem,
    load_sem,
    record_sem,
    send_sem,
    recv_sem,
    name_send_sem,
    name_recv_sem,
):
    nx, ny, nz = sizes
    devices = nx * ny * nz
    plane = nx * nz
    levels, slots = diag_ref.shape[:2]
    records = off_refs[0].shape[0]
    lanes = names_ref.shape[-1]
    groups = work_ref.shape[1]
    rows = TILE // groups
    pack = CAP * rows
    mx, my, mz = (lax.axis_index(axis) for axis in AXES)
    me = (mx * ny + my) * nz + mz

    def partner(index):
        at = index // plane
        down = ny - 1 - at
        down = down - jnp.where(down > my, 0, 1)
        up = at + jnp.where(at < my, 0, 1)
        oy = jnp.where(at == ny - 1, my, jnp.where(2 * my < ny, down, up))
        rest = index % plane + 1
        ox = lax.rem(mx + rest // nz, nx)
        oz = lax.rem(mz + rest % nz, nz)
        return (ox * ny + oy) * nz + oz, (ox, oy, oz)

    def over(count, body):
        whole = count // CHUNK if count > CHUNK else 0

        if whole:

            @pl.loop(0, whole)
            def _(chunk):
                for item in range(CHUNK):
                    body(chunk * CHUNK + item)

        for index in range(whole * CHUNK, count):
            body(index)

    def over_partners(body):
        over(devices - 1, body)

    smalls = [
        pltpu.make_async_copy(live_hbm, live_ref, small_sem.at[0]),
        pltpu.make_async_copy(source_hbm, source_ref, small_sem.at[1]),
        pltpu.make_async_copy(owner_hbm, owner_ref, small_sem.at[2]),
        pltpu.make_async_copy(block_hbm, block_ref, small_sem.at[3]),
    ]
    right_load = pltpu.make_async_copy(right_hbm, right_ref, load_sem.at[0])
    diag_loads = [
        pltpu.make_async_copy(diag_hbm.at[at], diag_ref.at[at], load_sem.at[1 + at])
        for at in range(levels)
    ]
    off_loads = [
        pltpu.make_async_copy(off_hbm.at[at], off_refs[at], load_sem.at[1 + levels + at])
        for at in range(levels - 1)
    ]
    barrier = pltpu.get_barrier_semaphore()

    for copy in reversed(smalls):
        copy.start()
    right_load.start()
    diag_loads[0].start()
    off_loads[0].start()

    def greet(index):
        pl.semaphore_signal(barrier, inc=1, device_id=partner(index)[1], device_id_type=MESH)

    over_partners(greet)
    for at in range(1, levels):
        diag_loads[at].start()
        if at < levels - 1:
            off_loads[at].start()

    tile_rows = lax.broadcasted_iota(jnp.int32, (TILE, lanes), 0)

    def spread(at):
        for group in range(groups):
            for slot in range(slots):
                base = (at * slots + slot) * TILE + group * rows
                value = None
                for r in reversed(range(rows)):
                    row = jnp.broadcast_to(right_ref[base + r : base + r + 1, :], (TILE, lanes))
                    value = row if value is None else jnp.where(tile_rows % rows == r, row, value)
                work_ref[at, group, slot * TILE : (slot + 1) * TILE, :] = value

    def solve(at, group, total):
        count = live_ref[0, at]
        for slot in range(slots):
            part = slice(slot * TILE, (slot + 1) * TILE)
            work = work_ref[at, group, part, :]
            if total is not None:
                work = work - total[part]
            solved = jnp.dot(
                work.astype(jnp.bfloat16), diag_ref[at, slot], preferred_element_type=jnp.float32
            )
            solved = jnp.where(slot < count, solved, jnp.float32(0.0))
            solved_ref[slot] = solved
            out_ref[at, slot] = jnp.where(tile_rows // rows == group, solved, out_ref[at, slot])

    def make(at, group):
        for record in range(records):
            picked = solved_ref[source_ref[at, record]].astype(jnp.bfloat16)
            made_ref[record] = jnp.dot(
                picked, off_refs[at][record], preferred_element_type=jnp.float32
            )

        def message(other):
            first, last = (made_ref[record_ref[other, at * CAP + c]] for c in range(CAP))
            return jnp.where(tile_rows % pack < rows, first, last)

        def place(tile):
            value = None
            for item in range(TILE // pack):
                part = message(partner(tile * (TILE // pack) + item)[0])
                value = part if item == 0 else jnp.where(tile_rows // pack < item, value, part)
            outgoing_ref[at, group, pl.ds(tile * TILE, TILE), :] = value

        over(devices * pack // TILE, place)
        arrived_ref[at, group, pl.ds(me * pack, pack), :] = message(me)[:pack]

    def send(at, group):
        def one(index):
            _, where = partner(index)
            pltpu.make_async_remote_copy(
                src_ref=outgoing_ref.at[at, group, pl.ds(index * pack, pack)],
                dst_ref=arrived_ref.at[at, group, pl.ds(me * pack, pack)],
                send_sem=send_sem.at[at, group],
                recv_sem=recv_sem.at[at, group],
                device_id=where,
                device_id_type=MESH,
            ).start()

        over_partners(one)

    def incoming(at, group):
        value = arrived_ref[at, group]
        high = value.astype(jnp.bfloat16)
        low = (value - high.astype(jnp.float32)).astype(jnp.bfloat16)
        return jnp.concatenate([high, low], axis=0)

    def pair_at(source, target):
        return sum(levels - 1 - at for at in range(source)) + target - source - 1

    def gather(source, target, values):
        placer = placer_ref[pair_at(source, target)]
        return jnp.dot(
            jnp.concatenate([placer, placer], axis=1), values, preferred_element_type=jnp.float32
        )

    smalls[2].wait()
    smalls[3].wait()
    owner_ids = lax.broadcasted_iota(jnp.int32, (devices, records), 0)
    record_ids = lax.broadcasted_iota(jnp.int32, (devices, records), 1)
    lane_ids = lax.broadcasted_iota(jnp.int32, (devices, lanes), 1)
    told = jnp.zeros((devices, lanes), jnp.float32)
    index = jnp.zeros((devices, lanes), jnp.int32)
    for at in range(levels - 1):
        hits = owner_ids == owner_ref[at : at + 1, :]
        block_row = (block_ref[at : at + 1, :] + 1).astype(jnp.float32)
        first = jnp.min(jnp.where(hits, record_ids, records - 1), axis=1, keepdims=True)
        last = jnp.max(jnp.where(hits, record_ids, 0), axis=1, keepdims=True)
        for copy_at, record in enumerate((first, last)):
            chosen = jnp.where(hits & (record_ids == record), block_row, 0.0)
            label = jnp.sum(chosen, axis=1, keepdims=True)
            told = jnp.where(lane_ids == at * CAP + copy_at, label, told)
            index = jnp.where(lane_ids == at * CAP + copy_at, record, index)
    record_vmem[...] = index
    record_copy = pltpu.make_async_copy(record_vmem, record_ref, record_sem)
    record_copy.start()
    names_out_ref[...] = told.reshape(devices, 1, lanes)
    names_ref[pl.ds(me, 1)] = names_out_ref[pl.ds(me, 1)]

    right_load.wait()
    spread(0)
    smalls[0].wait()
    smalls[1].wait()
    diag_loads[0].wait()
    off_loads[0].wait()
    record_copy.wait()

    solve(0, 0, None)
    make(0, 0)
    pl.semaphore_wait(barrier, devices - 1)

    def tell(index):
        other, where = partner(index)
        pltpu.make_async_remote_copy(
            src_ref=names_out_ref.at[pl.ds(other, 1)],
            dst_ref=names_ref.at[pl.ds(me, 1)],
            send_sem=name_send_sem,
            recv_sem=name_recv_sem,
            device_id=where,
            device_id_type=MESH,
        ).start()

    over_partners(tell)

    send(0, 0)

    @pl.loop(1, groups)
    def _(group):
        solve(0, group, None)
        make(0, group)
        send(0, group)

    for at in range(1, levels):
        spread(at)

    name_part = names_ref.at[pl.ds(0, devices - 1)]
    pltpu.make_async_copy(name_part, name_part, name_recv_sem).wait()
    width = devices * pack
    wanted = -(-(levels - 1) * CAP // 8) * 8
    pick = (
        lax.broadcasted_iota(jnp.int32, (wanted, lanes), 0)
        == lax.broadcasted_iota(jnp.int32, (wanted, lanes), 1)
    ).astype(jnp.float32)
    names = lax.dot_general(
        pick,
        names_ref[...].reshape(devices, lanes),
        (((1,), (1,)), ((), ())),
        preferred_element_type=jnp.float32,
        precision=lax.Precision.HIGHEST,
    )
    widen = (
        lax.broadcasted_iota(jnp.int32, (devices, width), 0)
        == lax.broadcasted_iota(jnp.int32, (devices, width), 1) // pack
    ).astype(jnp.float32)
    wide = jnp.dot(
        names, widen, preferred_element_type=jnp.float32, precision=lax.Precision.HIGHEST
    ).astype(jnp.int32)
    column = lax.broadcasted_iota(jnp.int32, (1, width), 1)
    height = slots * TILE
    row_ids = lax.broadcasted_iota(jnp.int32, (height, width), 0)
    same = row_ids % rows == lax.broadcasted_iota(jnp.int32, (height, width), 1) % rows
    slot_ids = row_ids // TILE
    for source in range(levels - 1):
        at = source * CAP
        label = wide[at : at + 1]
        for c in range(1, CAP):
            label = jnp.where(column % pack // rows == c, wide[at + c : at + c + 1], label)
        for target in range(source + 1, levels):
            hit = same & (slot_ids == label - (target * slots + 1))
            placer_ref[pair_at(source, target)] = hit.astype(jnp.float32).astype(jnp.bfloat16)

    for at in range(1, levels):
        diag_loads[at].wait()
        if at < levels - 1:
            off_loads[at].wait()

        @pl.loop(0, groups)
        def _(group):
            part = arrived_ref.at[at - 1, group, pl.ds(0, (devices - 1) * pack)]
            pltpu.make_async_copy(part, part, recv_sem.at[at - 1, group]).wait()
            values = incoming(at - 1, group)
            solve(at, group, gather(at - 1, at, values))
            if at < levels - 1:
                make(at, group)
                send(at, group)
                for target in range(at + 1, levels):
                    work_ref[target, group] = work_ref[target, group] - gather(
                        at - 1, target, values
                    )

    name_part = names_out_ref.at[pl.ds(0, devices - 1)]
    pltpu.make_async_copy(name_part, name_part, name_send_sem).wait()
    for at in range(levels - 1):
        for group in range(groups):
            part = outgoing_ref.at[at, group, pl.ds(0, (devices - 1) * pack)]
            pltpu.make_async_copy(part, part, send_sem.at[at, group]).wait()


def shards(
    sizes,
    right_side,
    diag_inverse,
    off_blocks,
    live_counts,
    source_slot,
    target_owner,
    target_block,
):
    levels, slots, rhs, width = right_side.shape
    records = off_blocks.shape[1]
    devices = sizes[0] * sizes[1] * sizes[2]
    lanes = 128
    pack = CAP * rhs // GROUPS
    pairs = levels * (levels - 1) // 2
    vmem = pl.BlockSpec(memory_space=pltpu.VMEM)
    anywhere = pl.BlockSpec(memory_space=pl.ANY)
    messages = (levels - 1, GROUPS, devices * pack, width)
    return pl.pallas_call(
        functools.partial(kernel, sizes),
        out_shape=pltpu.VMEM((levels, slots, rhs, width), jnp.float32),
        in_specs=[anywhere] * 7,
        out_specs=vmem,
        scratch_shapes=[
            pltpu.SMEM((1, levels), jnp.int32),
            pltpu.SMEM(source_slot.shape, jnp.int32),
            pltpu.VMEM(target_owner.shape, jnp.int32),
            pltpu.VMEM(target_block.shape, jnp.int32),
            pltpu.VMEM((levels * slots * rhs, width), jnp.float32),
            pltpu.VMEM((levels, GROUPS, slots * rhs, width), jnp.float32),
            pltpu.VMEM(diag_inverse.shape, diag_inverse.dtype),
            tuple(
                pltpu.VMEM(off_blocks.shape[1:], off_blocks.dtype) for _ in range(levels - 1)
            ),
            pltpu.VMEM((slots, rhs, width), jnp.float32),
            pltpu.VMEM((records, rhs, width), jnp.float32),
            pltpu.VMEM(messages, jnp.float32),
            pltpu.VMEM(messages, jnp.float32),
            pltpu.VMEM((pairs, slots * rhs, devices * pack), jnp.bfloat16),
            pltpu.VMEM((devices, 1, lanes), jnp.float32),
            pltpu.VMEM((devices, 1, lanes), jnp.float32),
            pltpu.VMEM((devices, lanes), jnp.int32),
            pltpu.SMEM((devices, lanes), jnp.int32),
            pltpu.SemaphoreType.DMA((4,)),
            pltpu.SemaphoreType.DMA((2 * levels,)),
            pltpu.SemaphoreType.DMA,
            pltpu.SemaphoreType.DMA((levels - 1, GROUPS)),
            pltpu.SemaphoreType.DMA((levels - 1, GROUPS)),
            pltpu.SemaphoreType.DMA,
            pltpu.SemaphoreType.DMA,
        ],
        compiler_params=pltpu.CompilerParams(
            collective_id=0, has_side_effects=True, vmem_limit_bytes=60 * 1024 * 1024
        ),
    )(
        live_counts.reshape(1, levels),
        source_slot,
        target_owner,
        target_block,
        right_side.reshape(levels * slots * rhs, width),
        diag_inverse,
        off_blocks,
    )


def solution(mesh):
    sizes = tuple(mesh.shape[axis] for axis in AXES)
    in_specs = (
        P(None, AXES, None, None),
        P(None, AXES, None, None),
        P(None, AXES, None, None),
        P(None, AXES),
        P(None, AXES),
        P(None, AXES),
        P(None, AXES),
    )
    return jax.shard_map(
        functools.partial(shards, sizes),
        mesh=mesh,
        in_specs=in_specs,
        out_specs=P(None, AXES, None, None),
        check_vma=False,
    )
```

```python
import functools

import jax
import jax.numpy as jnp
from jax import lax
from jax.experimental import pallas as pl
from jax.experimental.pallas import tpu as pltpu
from jax.sharding import PartitionSpec as P

CAP = 2
GROUPS = 4
TILE = 8
AXES = ("gx", "gy", "gz")
MESH = pl.DeviceIdType.MESH


def shifted(coord, offset, size):
    if size & (size - 1):
        return (coord + offset) % size
    for bit in range(size.bit_length() - 1):
        if offset >> bit & 1:
            coord = coord + (1 << bit) * (1 - 2 * (coord // (1 << bit) % 2))
    return coord


def kernel(
    sizes,
    live_hbm,
    source_hbm,
    owner_hbm,
    block_hbm,
    right_hbm,
    diag_hbm,
    off_hbm,
    out_ref,
    live_ref,
    source_ref,
    owner_ref,
    block_ref,
    right_ref,
    work_ref,
    diag_ref,
    off_ref,
    solved_ref,
    made_ref,
    outgoing_ref,
    arrived_ref,
    placer_ref,
    names_out_ref,
    names_ref,
    record_vmem,
    record_ref,
    small_sem,
    load_sem,
    send_sem,
    recv_sem,
    name_send_sem,
    name_recv_sem,
):
    nx, ny, nz = sizes
    devices = nx * ny * nz
    levels, slots = diag_ref.shape[:2]
    records = off_ref.shape[1]
    lanes = names_ref.shape[-1]
    groups = work_ref.shape[1]
    rows = TILE // groups
    pack = CAP * rows
    mx, my, mz = (lax.axis_index(axis) for axis in AXES)
    me = (mx * ny + my) * nz + mz

    coords = [[shifted(m, d, n) for d in range(n)] for m, n in zip((mx, my, mz), sizes)]
    offsets = sorted(
        [(dx, dy, dz) for dx in range(nx) for dy in range(ny) for dz in range(nz)],
        key=lambda o: (-o[1].bit_count() - (o[1] > 2) - o[0].bit_count(), -o[1], -o[0], -o[2]),
    )

    def partner(index):
        where = tuple(coord[d] for coord, d in zip(coords, offsets[index]))
        return (where[0] * ny + where[1]) * nz + where[2], where

    def over(count, body):
        for index in range(count):
            body(index)

    def over_partners(body):
        over(devices - 1, body)

    smalls = [
        pltpu.make_async_copy(live_hbm, live_ref, small_sem.at[0]),
        pltpu.make_async_copy(source_hbm, source_ref, small_sem.at[1]),
        pltpu.make_async_copy(owner_hbm, owner_ref, small_sem.at[2]),
        pltpu.make_async_copy(block_hbm, block_ref, small_sem.at[3]),
    ]
    right_load = pltpu.make_async_copy(right_hbm, right_ref, load_sem.at[0])
    first_loads, rest_loads = (
        [
            pltpu.make_async_copy(hbm.at[part], ref.at[part], load_sem.at[1 + i])
            for i, (hbm, ref, count) in enumerate(
                ((diag_hbm, diag_ref, levels), (off_hbm, off_ref, levels - 1))
            )
            for part in (pl.ds(begin, 1 if begin == 0 else count - 1),)
        ]
        for begin in (0, 1)
    )
    barrier = pltpu.get_barrier_semaphore()

    def greet(index):
        pl.semaphore_signal(barrier, inc=1, device_id=partner(index)[1], device_id_type=MESH)

    for copy in reversed(smalls):
        copy.start()
    right_load.start()
    for copy in first_loads:
        copy.start()
    over_partners(greet)
    tile_rows = lax.broadcasted_iota(jnp.int32, (TILE, lanes), 0)

    def spread(at):
        for group in range(groups):
            for slot in range(slots):
                base = (at * slots + slot) * TILE + group * rows
                value = None
                for r in reversed(range(rows)):
                    row = jnp.broadcast_to(right_ref[base + r : base + r + 1, :], (TILE, lanes))
                    value = row if value is None else jnp.where(tile_rows % rows == r, row, value)
                work_ref[at, group, slot * TILE : (slot + 1) * TILE, :] = value

    def solve(at, group, total):
        count = live_ref[0, at]
        for slot in range(slots):
            part = slice(slot * TILE, (slot + 1) * TILE)
            work = work_ref[at, group, part, :]
            if total is not None:
                work = work - total[part]
            solved = jnp.dot(
                work.astype(jnp.bfloat16), diag_ref[at, slot], preferred_element_type=jnp.float32
            )
            solved = jnp.where(slot < count, solved, jnp.float32(0.0))
            solved_ref[slot] = solved
            out_ref[at, slot] = jnp.where(tile_rows // rows == group, solved, out_ref[at, slot])

    def make(at, group, awaited=None):
        for record in range(records):
            picked = solved_ref[source_ref[at, record]].astype(jnp.bfloat16)
            made_ref[record] = jnp.dot(
                picked, off_ref[at, record], preferred_element_type=jnp.float32
            )

        if awaited is not None:
            awaited.wait()

        def message(other):
            first, last = (made_ref[record_ref[other, at * CAP + c]] for c in range(CAP))
            return jnp.where(tile_rows % pack < rows, first, last)

        def place(tile):
            value = None
            for item in range(TILE // pack):
                part = message(partner(tile * (TILE // pack) + item)[0])
                value = part if item == 0 else jnp.where(tile_rows // pack < item, value, part)
            outgoing_ref[at, group, pl.ds(tile * TILE, TILE), :] = value

        over(devices * pack // TILE, place)
        arrived_ref[at, group, pl.ds(me * pack, pack), :] = message(me)[:pack]

    def send(at, group):
        def one(index):
            _, where = partner(index)
            pltpu.make_async_remote_copy(
                src_ref=outgoing_ref.at[at, group, pl.ds(index * pack, pack)],
                dst_ref=arrived_ref.at[at, group, pl.ds(me * pack, pack)],
                send_sem=send_sem.at[group],
                recv_sem=recv_sem.at[at % 2, group],
                device_id=where,
                device_id_type=MESH,
            ).start()

        over_partners(one)

    def incoming(at, group):
        value = arrived_ref[at, group]
        high = value.astype(jnp.bfloat16)
        low = (value - high.astype(jnp.float32)).astype(jnp.bfloat16)
        return jnp.concatenate([high, low], axis=0)

    def pair_at(source, target):
        return sum(levels - 1 - at for at in range(source)) + target - source - 1

    def gather(source, target, values):
        placer = placer_ref[pair_at(source, target)]
        return jnp.dot(
            jnp.concatenate([placer, placer], axis=1), values, preferred_element_type=jnp.float32
        )

    smalls[2].wait()
    smalls[3].wait()
    owner_ids = lax.broadcasted_iota(jnp.int32, (devices, records), 0)
    record_ids = lax.broadcasted_iota(jnp.int32, (devices, records), 1)
    lane_ids = lax.broadcasted_iota(jnp.int32, (devices, lanes), 1)
    told = jnp.zeros((devices, lanes), jnp.float32)
    index = jnp.zeros((devices, lanes), jnp.int32)
    for at in range(levels - 1):
        hits = owner_ids == owner_ref[at : at + 1, :]
        block_row = (block_ref[at : at + 1, :] + 1).astype(jnp.float32)
        first = jnp.min(jnp.where(hits, record_ids, records - 1), axis=1, keepdims=True)
        last = jnp.max(jnp.where(hits, record_ids, 0), axis=1, keepdims=True)
        for copy_at, record in enumerate((first, last)):
            chosen = jnp.where(hits & (record_ids == record), block_row, 0.0)
            label = jnp.sum(chosen, axis=1, keepdims=True)
            told = jnp.where(lane_ids == at * CAP + copy_at, label, told)
            index = jnp.where(lane_ids == at * CAP + copy_at, record, index)
    record_vmem[...] = index
    record_copy = pltpu.make_async_copy(record_vmem, record_ref, small_sem.at[2])
    record_copy.start()
    names_out_ref[...] = told.reshape(devices, 1, lanes)
    names_ref[pl.ds(me, 1)] = names_out_ref[pl.ds(me, 1)]

    right_load.wait()
    spread(0)
    smalls[0].wait()
    smalls[1].wait()
    for copy in first_loads:
        copy.wait()
    for copy in rest_loads:
        copy.start()

    solve(0, 0, None)
    make(0, 0, record_copy)
    pl.semaphore_wait(barrier, devices - 1)

    def tell(index):
        other, where = partner(index)
        pltpu.make_async_remote_copy(
            src_ref=names_out_ref.at[pl.ds(other, 1)],
            dst_ref=names_ref.at[pl.ds(me, 1)],
            send_sem=name_send_sem,
            recv_sem=name_recv_sem,
            device_id=where,
            device_id_type=MESH,
        ).start()

    over_partners(tell)

    send(0, 0)

    @pl.loop(1, groups)
    def _(group):
        solve(0, group, None)
        make(0, group)
        send(0, group)

    for at in range(1, levels):
        spread(at)

    name_part = names_ref.at[pl.ds(0, devices - 1)]
    pltpu.make_async_copy(name_part, name_part, name_recv_sem).wait()
    width = devices * pack
    wanted = -(-(levels - 1) * CAP // 8) * 8
    pick = (
        lax.broadcasted_iota(jnp.int32, (wanted, lanes), 0)
        == lax.broadcasted_iota(jnp.int32, (wanted, lanes), 1)
    ).astype(jnp.float32)
    names = lax.dot_general(
        pick,
        names_ref[...].reshape(devices, lanes),
        (((1,), (1,)), ((), ())),
        preferred_element_type=jnp.float32,
    )
    widen = (
        lax.broadcasted_iota(jnp.int32, (devices, width), 0)
        == lax.broadcasted_iota(jnp.int32, (devices, width), 1) // pack
    ).astype(jnp.float32)
    wide = jnp.dot(names, widen, preferred_element_type=jnp.float32).astype(jnp.int32)
    column = lax.broadcasted_iota(jnp.int32, (1, width), 1)
    height = slots * TILE
    row_ids = lax.broadcasted_iota(jnp.int32, (height, width), 0)
    same = row_ids % rows == lax.broadcasted_iota(jnp.int32, (height, width), 1) % rows
    slot_ids = row_ids // TILE

    def build(source):
        at = source * CAP
        label = wide[at : at + 1]
        for c in range(1, CAP):
            label = jnp.where(column % pack // rows == c, wide[at + c : at + c + 1], label)
        for target in range(source + 1, levels):
            hit = same & (slot_ids == label - (target * slots + 1))
            placer_ref[pair_at(source, target)] = hit.astype(jnp.float32).astype(jnp.bfloat16)

    build(0)
    for copy in rest_loads:
        copy.wait()
    name_part = names_out_ref.at[pl.ds(0, devices - 1)]
    pltpu.make_async_copy(name_part, name_part, name_send_sem).wait()
    for at in range(1, levels):
        if at < levels - 1:
            build(at)
        @pl.loop(0, groups)
        def _(group):
            part = arrived_ref.at[at - 1, group, pl.ds(0, (devices - 1) * pack)]
            pltpu.make_async_copy(part, part, recv_sem.at[(at - 1) % 2, group]).wait()
            values = incoming(at - 1, group)
            total = gather(at - 1, at, values)
            for target in range(at + 1, levels):
                work_ref[target, group] = work_ref[target, group] - gather(
                    at - 1, target, values
                )
            solve(at, group, total)
            part = outgoing_ref.at[at - 1, group, pl.ds(0, (devices - 1) * pack)]
            pltpu.make_async_copy(part, part, send_sem.at[group]).wait()
            if at < levels - 1:
                make(at, group)
                send(at, group)


def shards(
    sizes,
    right_side,
    diag_inverse,
    off_blocks,
    live_counts,
    source_slot,
    target_owner,
    target_block,
):
    levels, slots, rhs, width = right_side.shape
    records = off_blocks.shape[1]
    devices = sizes[0] * sizes[1] * sizes[2]
    lanes = 128
    pack = CAP * rhs // GROUPS
    pairs = levels * (levels - 1) // 2
    vmem = pl.BlockSpec(memory_space=pltpu.VMEM)
    anywhere = pl.BlockSpec(memory_space=pl.ANY)
    messages = (levels - 1, GROUPS, devices * pack, width)
    return pl.pallas_call(
        functools.partial(kernel, sizes),
        out_shape=pltpu.VMEM((levels, slots, rhs, width), jnp.float32),
        in_specs=[anywhere] * 7,
        out_specs=vmem,
        scratch_shapes=[
            pltpu.SMEM((1, levels), jnp.int32),
            pltpu.SMEM(source_slot.shape, jnp.int32),
            pltpu.VMEM(target_owner.shape, jnp.int32),
            pltpu.VMEM(target_block.shape, jnp.int32),
            pltpu.VMEM((levels * slots * rhs, width), jnp.float32),
            pltpu.VMEM((levels, GROUPS, slots * rhs, width), jnp.float32),
            pltpu.VMEM(diag_inverse.shape, diag_inverse.dtype),
            pltpu.VMEM(off_blocks.shape, off_blocks.dtype),
            pltpu.VMEM((slots, rhs, width), jnp.float32),
            pltpu.VMEM((records, rhs, width), jnp.float32),
            pltpu.VMEM(messages, jnp.float32),
            pltpu.VMEM(messages, jnp.float32),
            pltpu.VMEM((pairs, slots * rhs, devices * pack), jnp.bfloat16),
            pltpu.VMEM((devices, 1, lanes), jnp.float32),
            pltpu.VMEM((devices, 1, lanes), jnp.float32),
            pltpu.VMEM((devices, lanes), jnp.int32),
            pltpu.SMEM((devices, lanes), jnp.int32),
            pltpu.SemaphoreType.DMA((4,)),
            pltpu.SemaphoreType.DMA((3,)),
            pltpu.SemaphoreType.DMA((GROUPS,)),
            pltpu.SemaphoreType.DMA((2, GROUPS)),
            pltpu.SemaphoreType.DMA,
            pltpu.SemaphoreType.DMA,
        ],
        compiler_params=pltpu.CompilerParams(
            collective_id=0, has_side_effects=True, vmem_limit_bytes=60 * 1024 * 1024
        ),
    )(
        live_counts.reshape(1, levels),
        source_slot,
        target_owner,
        target_block,
        right_side.reshape(levels * slots * rhs, width),
        diag_inverse,
        off_blocks,
    )


def solution(mesh):
    sizes = tuple(mesh.shape[axis] for axis in AXES)
    in_specs = (
        P(None, AXES, None, None),
        P(None, AXES, None, None),
        P(None, AXES, None, None),
        P(None, AXES),
        P(None, AXES),
        P(None, AXES),
        P(None, AXES),
    )
    return jax.shard_map(
        functools.partial(shards, sizes),
        mesh=mesh,
        in_specs=in_specs,
        out_specs=P(None, AXES, None, None),
        check_vma=False,
    )
```

```python
import functools

import jax
import jax.numpy as jnp
from jax import lax
from jax.experimental import pallas as pl
from jax.experimental.pallas import tpu as pltpu
from jax.sharding import PartitionSpec as P

CAP = 2
GROUPS = 4
TILE = 8
AXES = ("gx", "gy", "gz")
MESH = pl.DeviceIdType.MESH


def shifted(coord, offset, size):
    if size & (size - 1):
        return (coord + offset) % size
    for bit in range(size.bit_length() - 1):
        if offset >> bit & 1:
            coord = coord + (1 << bit) * (1 - 2 * (coord // (1 << bit) % 2))
    return coord


def kernel(
    sizes,
    live_hbm,
    source_hbm,
    owner_hbm,
    block_hbm,
    right_hbm,
    diag_hbm,
    off_hbm,
    out_ref,
    live_ref,
    source_ref,
    owner_ref,
    block_ref,
    right_ref,
    work_ref,
    diag_ref,
    off_ref,
    solved_ref,
    made_ref,
    outgoing_ref,
    arrived_ref,
    placer_ref,
    names_out_ref,
    names_ref,
    record_vmem,
    record_ref,
    small_sem,
    load_sem,
    send_sem,
    recv_sem,
    name_send_sem,
    name_recv_sem,
):
    nx, ny, nz = sizes
    devices = nx * ny * nz
    levels, slots = diag_ref.shape[:2]
    records = off_ref.shape[1]
    lanes = names_ref.shape[-1]
    groups = work_ref.shape[1]
    rows = TILE // groups
    pack = CAP * rows
    mx, my, mz = (lax.axis_index(axis) for axis in AXES)
    me = (mx * ny + my) * nz + mz

    coords = [[shifted(m, d, n) for d in range(n)] for m, n in zip((mx, my, mz), sizes)]
    offsets = sorted(
        [(dx, dy, dz) for dx in range(nx) for dy in range(ny) for dz in range(nz)],
        key=lambda o: (-min(o[1], 2) - o[0].bit_count(), -o[1], -o[0], -o[2]),
    )

    def partner(index):
        where = tuple(coord[d] for coord, d in zip(coords, offsets[index]))
        return (where[0] * ny + where[1]) * nz + where[2], where

    def over(count, body):
        for index in range(count):
            body(index)

    def over_partners(body):
        over(devices - 1, body)

    smalls = [
        pltpu.make_async_copy(live_hbm, live_ref, small_sem.at[0]),
        pltpu.make_async_copy(source_hbm, source_ref, small_sem.at[1]),
        pltpu.make_async_copy(owner_hbm, owner_ref, small_sem.at[2]),
        pltpu.make_async_copy(block_hbm, block_ref, small_sem.at[3]),
    ]
    right_load = pltpu.make_async_copy(right_hbm, right_ref, load_sem.at[0])
    first_loads, rest_loads = (
        [
            pltpu.make_async_copy(hbm.at[part], ref.at[part], load_sem.at[1 + i])
            for i, (hbm, ref, count) in enumerate(
                ((diag_hbm, diag_ref, levels), (off_hbm, off_ref, levels - 1))
            )
            for part in (pl.ds(begin, 1 if begin == 0 else count - 1),)
        ]
        for begin in (0, 1)
    )
    barrier = pltpu.get_barrier_semaphore()

    def greet(index):
        pl.semaphore_signal(barrier, inc=1, device_id=partner(index)[1], device_id_type=MESH)

    for copy in reversed(smalls):
        copy.start()
    right_load.start()
    for copy in first_loads:
        copy.start()
    over_partners(greet)
    tile_rows = lax.broadcasted_iota(jnp.int32, (TILE, lanes), 0)

    def spread(at):
        for group in range(groups):
            for slot in range(slots):
                base = (at * slots + slot) * TILE + group * rows
                value = None
                for r in reversed(range(rows)):
                    row = jnp.broadcast_to(right_ref[base + r : base + r + 1, :], (TILE, lanes))
                    value = row if value is None else jnp.where(tile_rows % rows == r, row, value)
                work_ref[at, group, slot * TILE : (slot + 1) * TILE, :] = value

    def solve(at, group, total):
        count = live_ref[0, at]
        for slot in range(slots):
            part = slice(slot * TILE, (slot + 1) * TILE)
            work = work_ref[at, group, part, :]
            if total is not None:
                work = work - total[part]
            solved = jnp.dot(
                work.astype(jnp.bfloat16), diag_ref[at, slot], preferred_element_type=jnp.float32
            )
            solved = jnp.where(slot < count, solved, jnp.float32(0.0))
            solved_ref[slot] = solved
            out_ref[at, slot] = jnp.where(tile_rows // rows == group, solved, out_ref[at, slot])

    def make(at, group, awaited=None):
        for record in range(records):
            picked = solved_ref[source_ref[at, record]].astype(jnp.bfloat16)
            made_ref[record] = jnp.dot(
                picked, off_ref[at, record], preferred_element_type=jnp.float32
            )

        if awaited is not None:
            awaited.wait()

        def message(other):
            first, last = (made_ref[record_ref[other, at * CAP + c]] for c in range(CAP))
            return jnp.where(tile_rows % pack < rows, first, last)

        def place(tile):
            value = None
            for item in range(TILE // pack):
                part = message(partner(tile * (TILE // pack) + item)[0])
                value = part if item == 0 else jnp.where(tile_rows // pack < item, value, part)
            outgoing_ref[at, group, pl.ds(tile * TILE, TILE), :] = value

        over(devices * pack // TILE, place)
        arrived_ref[at, group, pl.ds(me * pack, pack), :] = message(me)[:pack]

    def send(at, group):
        def one(index):
            _, where = partner(index)
            pltpu.make_async_remote_copy(
                src_ref=outgoing_ref.at[at, group, pl.ds(index * pack, pack)],
                dst_ref=arrived_ref.at[at, group, pl.ds(me * pack, pack)],
                send_sem=send_sem.at[group],
                recv_sem=recv_sem.at[at % 2, group],
                device_id=where,
                device_id_type=MESH,
            ).start()

        over_partners(one)

    def incoming(at, group):
        value = arrived_ref[at, group]
        high = value.astype(jnp.bfloat16)
        low = (value - high.astype(jnp.float32)).astype(jnp.bfloat16)
        return jnp.concatenate([high, low], axis=0)

    def pair_at(source, target):
        return sum(levels - 1 - at for at in range(source)) + target - source - 1

    def gather(source, target, values):
        placer = placer_ref[pair_at(source, target)]
        return jnp.dot(
            jnp.concatenate([placer, placer], axis=1), values, preferred_element_type=jnp.float32
        )

    smalls[2].wait()
    smalls[3].wait()
    owner_ids = lax.broadcasted_iota(jnp.int32, (devices, records), 0)
    record_ids = lax.broadcasted_iota(jnp.int32, (devices, records), 1)
    lane_ids = lax.broadcasted_iota(jnp.int32, (devices, lanes), 1)
    told = jnp.zeros((devices, lanes), jnp.float32)
    index = jnp.zeros((devices, lanes), jnp.int32)
    for at in range(levels - 1):
        hits = owner_ids == owner_ref[at : at + 1, :]
        block_row = (block_ref[at : at + 1, :] + 1).astype(jnp.float32)
        first = jnp.min(jnp.where(hits, record_ids, records - 1), axis=1, keepdims=True)
        last = jnp.max(jnp.where(hits, record_ids, 0), axis=1, keepdims=True)
        for copy_at, record in enumerate((first, last)):
            chosen = jnp.where(hits & (record_ids == record), block_row, 0.0)
            label = jnp.sum(chosen, axis=1, keepdims=True)
            told = jnp.where(lane_ids == at * CAP + copy_at, label, told)
            index = jnp.where(lane_ids == at * CAP + copy_at, record, index)
    record_vmem[...] = index
    record_copy = pltpu.make_async_copy(record_vmem, record_ref, small_sem.at[2])
    record_copy.start()
    names_out_ref[...] = told.reshape(devices, 1, lanes)
    names_ref[pl.ds(me, 1)] = names_out_ref[pl.ds(me, 1)]

    right_load.wait()
    spread(0)
    smalls[0].wait()
    smalls[1].wait()
    for copy in first_loads:
        copy.wait()
    for copy in rest_loads:
        copy.start()

    solve(0, 0, None)
    make(0, 0, record_copy)
    pl.semaphore_wait(barrier, devices - 1)

    def tell(index):
        other, where = partner(index)
        pltpu.make_async_remote_copy(
            src_ref=names_out_ref.at[pl.ds(other, 1)],
            dst_ref=names_ref.at[pl.ds(me, 1)],
            send_sem=name_send_sem,
            recv_sem=name_recv_sem,
            device_id=where,
            device_id_type=MESH,
        ).start()

    over_partners(tell)

    send(0, 0)

    @pl.loop(1, groups)
    def _(group):
        solve(0, group, None)
        make(0, group)
        send(0, group)

    for at in range(1, levels):
        spread(at)

    name_part = names_ref.at[pl.ds(0, devices - 1)]
    pltpu.make_async_copy(name_part, name_part, name_recv_sem).wait()
    width = devices * pack
    wanted = -(-(levels - 1) * CAP // 8) * 8
    pick = (
        lax.broadcasted_iota(jnp.int32, (wanted, lanes), 0)
        == lax.broadcasted_iota(jnp.int32, (wanted, lanes), 1)
    ).astype(jnp.float32)
    names = lax.dot_general(
        pick,
        names_ref[...].reshape(devices, lanes),
        (((1,), (1,)), ((), ())),
        preferred_element_type=jnp.float32,
    )
    widen = (
        lax.broadcasted_iota(jnp.int32, (devices, width), 0)
        == lax.broadcasted_iota(jnp.int32, (devices, width), 1) // pack
    ).astype(jnp.float32)
    wide = jnp.dot(names, widen, preferred_element_type=jnp.float32).astype(jnp.int32)
    column = lax.broadcasted_iota(jnp.int32, (1, width), 1)
    height = slots * TILE
    row_ids = lax.broadcasted_iota(jnp.int32, (height, width), 0)
    same = row_ids % rows == lax.broadcasted_iota(jnp.int32, (height, width), 1) % rows
    slot_ids = row_ids // TILE

    def build(source):
        at = source * CAP
        label = wide[at : at + 1]
        for c in range(1, CAP):
            label = jnp.where(column % pack // rows == c, wide[at + c : at + c + 1], label)
        for target in range(source + 1, levels):
            hit = same & (slot_ids == label - (target * slots + 1))
            placer_ref[pair_at(source, target)] = hit.astype(jnp.float32).astype(jnp.bfloat16)

    build(0)
    for copy in rest_loads:
        copy.wait()
    name_part = names_out_ref.at[pl.ds(0, devices - 1)]
    pltpu.make_async_copy(name_part, name_part, name_send_sem).wait()
    for at in range(1, levels):
        if at < levels - 1:
            build(at)
        @pl.loop(0, groups)
        def _(group):
            part = arrived_ref.at[at - 1, group, pl.ds(0, (devices - 1) * pack)]
            pltpu.make_async_copy(part, part, recv_sem.at[(at - 1) % 2, group]).wait()
            values = incoming(at - 1, group)
            total = gather(at - 1, at, values)
            for target in range(at + 1, levels):
                work_ref[target, group] = work_ref[target, group] - gather(
                    at - 1, target, values
                )
            solve(at, group, total)
            part = outgoing_ref.at[at - 1, group, pl.ds(0, (devices - 1) * pack)]
            pltpu.make_async_copy(part, part, send_sem.at[group]).wait()
            if at < levels - 1:
                make(at, group)
                send(at, group)


def shards(
    sizes,
    right_side,
    diag_inverse,
    off_blocks,
    live_counts,
    source_slot,
    target_owner,
    target_block,
):
    levels, slots, rhs, width = right_side.shape
    records = off_blocks.shape[1]
    devices = sizes[0] * sizes[1] * sizes[2]
    lanes = 128
    pack = CAP * rhs // GROUPS
    pairs = levels * (levels - 1) // 2
    vmem = pl.BlockSpec(memory_space=pltpu.VMEM)
    anywhere = pl.BlockSpec(memory_space=pl.ANY)
    messages = (levels - 1, GROUPS, devices * pack, width)
    return pl.pallas_call(
        functools.partial(kernel, sizes),
        out_shape=pltpu.VMEM((levels, slots, rhs, width), jnp.float32),
        in_specs=[anywhere] * 7,
        out_specs=vmem,
        scratch_shapes=[
            pltpu.SMEM((1, levels), jnp.int32),
            pltpu.SMEM(source_slot.shape, jnp.int32),
            pltpu.VMEM(target_owner.shape, jnp.int32),
            pltpu.VMEM(target_block.shape, jnp.int32),
            pltpu.VMEM((levels * slots * rhs, width), jnp.float32),
            pltpu.VMEM((levels, GROUPS, slots * rhs, width), jnp.float32),
            pltpu.VMEM(diag_inverse.shape, diag_inverse.dtype),
            pltpu.VMEM(off_blocks.shape, off_blocks.dtype),
            pltpu.VMEM((slots, rhs, width), jnp.float32),
            pltpu.VMEM((records, rhs, width), jnp.float32),
            pltpu.VMEM(messages, jnp.float32),
            pltpu.VMEM(messages, jnp.float32),
            pltpu.VMEM((pairs, slots * rhs, devices * pack), jnp.bfloat16),
            pltpu.VMEM((devices, 1, lanes), jnp.float32),
            pltpu.VMEM((devices, 1, lanes), jnp.float32),
            pltpu.VMEM((devices, lanes), jnp.int32),
            pltpu.SMEM((devices, lanes), jnp.int32),
            pltpu.SemaphoreType.DMA((4,)),
            pltpu.SemaphoreType.DMA((3,)),
            pltpu.SemaphoreType.DMA((GROUPS,)),
            pltpu.SemaphoreType.DMA((2, GROUPS)),
            pltpu.SemaphoreType.DMA,
            pltpu.SemaphoreType.DMA,
        ],
        compiler_params=pltpu.CompilerParams(
            collective_id=0, has_side_effects=True, vmem_limit_bytes=60 * 1024 * 1024
        ),
    )(
        live_counts.reshape(1, levels),
        source_slot,
        target_owner,
        target_block,
        right_side.reshape(levels * slots * rhs, width),
        diag_inverse,
        off_blocks,
    )


def solution(mesh):
    sizes = tuple(mesh.shape[axis] for axis in AXES)
    in_specs = (
        P(None, AXES, None, None),
        P(None, AXES, None, None),
        P(None, AXES, None, None),
        P(None, AXES),
        P(None, AXES),
        P(None, AXES),
        P(None, AXES),
    )
    return jax.shard_map(
        functools.partial(shards, sizes),
        mesh=mesh,
        in_specs=in_specs,
        out_specs=P(None, AXES, None, None),
        check_vma=False,
    )
```

```python
import functools

import jax
import jax.numpy as jnp
from jax import lax
from jax.experimental import pallas as pl
from jax.experimental.pallas import tpu as pltpu
from jax.sharding import PartitionSpec as P

CAP = 2
GROUPS = 4
BATCH = 8
TILE = 8
AXES = ("gx", "gy", "gz")
MESH = pl.DeviceIdType.MESH


def shifted(coord, offset, size):
    if size & (size - 1):
        return (coord + offset) % size
    for bit in range(size.bit_length() - 1):
        if offset >> bit & 1:
            coord = coord + (1 << bit) * (1 - 2 * (coord // (1 << bit) % 2))
    return coord


def kernel(
    sizes,
    live_hbm,
    source_hbm,
    owner_hbm,
    block_hbm,
    right_hbm,
    diag_hbm,
    off_hbm,
    out_ref,
    live_ref,
    source_ref,
    owner_ref,
    block_ref,
    right_ref,
    work_ref,
    diag_ref,
    off_ref,
    solved_ref,
    made_ref,
    outgoing_ref,
    arrived_ref,
    placer_ref,
    names_out_ref,
    names_ref,
    record_vmem,
    record_ref,
    small_sem,
    load_sem,
    send_sem,
    recv_sem,
    name_recv_sem,
):
    nx, ny, nz = sizes
    devices = nx * ny * nz
    levels, slots = diag_ref.shape[:2]
    records = off_ref.shape[1]
    lanes = names_ref.shape[-1]
    groups = work_ref.shape[1]
    rows = TILE // groups
    pack = CAP * rows
    mx, my, mz = (lax.axis_index(axis) for axis in AXES)
    me = (mx * ny + my) * nz + mz

    coords = [[shifted(m, d, n) for d in range(n)] for m, n in zip((mx, my, mz), sizes)]
    offsets = sorted(
        [(dx, dy, dz) for dx in range(nx) for dy in range(ny) for dz in range(nz)],
        key=lambda o: (-min(o[1], 2) - o[0].bit_count(), -o[1], -o[0], -o[2]),
    )

    def partner(index):
        where = tuple(coord[d] for coord, d in zip(coords, offsets[index]))
        return (where[0] * ny + where[1]) * nz + where[2], where

    def over(count, body):
        for index in range(count):
            body(index)

    def over_partners(body):
        over(devices - 1, body)

    smalls = [
        pltpu.make_async_copy(live_hbm, live_ref, small_sem.at[0]),
        pltpu.make_async_copy(source_hbm, source_ref, small_sem.at[1]),
        pltpu.make_async_copy(owner_hbm, owner_ref, small_sem.at[2]),
        pltpu.make_async_copy(block_hbm, block_ref, small_sem.at[3]),
    ]
    right_load = pltpu.make_async_copy(right_hbm, right_ref, load_sem.at[0])
    first_loads, rest_loads = (
        [
            pltpu.make_async_copy(hbm.at[part], ref.at[part], load_sem.at[1 + i])
            for i, (hbm, ref, count) in enumerate(
                ((diag_hbm, diag_ref, levels), (off_hbm, off_ref, levels - 1))
            )
            for part in (pl.ds(begin, 1 if begin == 0 else count - 1),)
        ]
        for begin in (0, 1)
    )
    barrier = pltpu.get_barrier_semaphore()

    def greet(index):
        pl.semaphore_signal(barrier, inc=1, device_id=partner(index)[1], device_id_type=MESH)

    for copy in reversed(smalls):
        copy.start()
    right_load.start()
    for copy in first_loads:
        copy.start()
    over_partners(greet)
    tile_rows = lax.broadcasted_iota(jnp.int32, (TILE, lanes), 0)

    def spread(at):
        for group in range(groups):
            for slot in range(slots):
                base = (at * slots + slot) * TILE + group * rows
                value = None
                for r in reversed(range(rows)):
                    row = jnp.broadcast_to(right_ref[base + r : base + r + 1, :], (TILE, lanes))
                    value = row if value is None else jnp.where(tile_rows % rows == r, row, value)
                work_ref[at, group, slot * TILE : (slot + 1) * TILE, :] = value

    def solve(at, group, total):
        count = live_ref[0, at]
        for slot in range(slots):
            part = slice(slot * TILE, (slot + 1) * TILE)
            work = work_ref[at, group, part, :]
            if total is not None:
                work = work - total[part]
            solved = jnp.dot(
                work.astype(jnp.bfloat16), diag_ref[at, slot], preferred_element_type=jnp.float32
            )
            solved = jnp.where(slot < count, solved, jnp.float32(0.0))
            solved_ref[slot] = solved
            out_ref[at, slot] = jnp.where(tile_rows // rows == group, solved, out_ref[at, slot])

    def make(at, group, awaited=None):
        for record in range(records):
            picked = solved_ref[source_ref[at, record]].astype(jnp.bfloat16)
            made_ref[record] = jnp.dot(
                picked, off_ref[at, record], preferred_element_type=jnp.float32
            )

        if awaited is not None:
            awaited.wait()

        def message(other):
            first, last = (made_ref[record_ref[other, at * CAP + c]] for c in range(CAP))
            return jnp.where(tile_rows % pack < rows, first, last)

        def place(tile):
            value = None
            for item in range(TILE // pack):
                part = message(partner(tile * (TILE // pack) + item)[0])
                value = part if item == 0 else jnp.where(tile_rows // pack < item, value, part)
            outgoing_ref[at, group, pl.ds(tile * TILE, TILE), :] = value

        return place, message

    def keep(at, group, message):
        arrived_ref[at, group, pl.ds(me * pack, pack), :] = message(me)[:pack]

    def deliver(at, group, place, message):
        step = BATCH
        each = TILE // pack
        for begin in range(0, devices, step):
            for tile in range(begin // each, (begin + step) // each):
                place(tile)
            if begin + step >= devices:
                keep(at, group, message)
            for index in range(begin, min(begin + step, devices - 1)):
                send_one(at, group, index)

    def send(at, group):
        over_partners(functools.partial(send_one, at, group))

    def send_one(at, group, index):
        _, where = partner(index)
        pltpu.make_async_remote_copy(
            src_ref=outgoing_ref.at[at, group, pl.ds(index * pack, pack)],
            dst_ref=arrived_ref.at[at, group, pl.ds(me * pack, pack)],
            send_sem=send_sem.at[group],
            recv_sem=recv_sem.at[at % 2, group],
            device_id=where,
            device_id_type=MESH,
        ).start()

    def incoming(at, group):
        value = arrived_ref[at, group]
        high = value.astype(jnp.bfloat16)
        low = (value - high.astype(jnp.float32)).astype(jnp.bfloat16)
        return jnp.concatenate([high, low], axis=0)

    def pair_at(source, target):
        return sum(levels - 1 - at for at in range(source)) + target - source - 1

    def gather(source, target, values):
        placer = placer_ref[pair_at(source, target)]
        return jnp.dot(
            jnp.concatenate([placer, placer], axis=1), values, preferred_element_type=jnp.float32
        )

    smalls[2].wait()
    smalls[3].wait()
    owner_ids = lax.broadcasted_iota(jnp.int32, (devices, records), 0)
    record_ids = lax.broadcasted_iota(jnp.int32, (devices, records), 1)
    lane_ids = lax.broadcasted_iota(jnp.int32, (devices, lanes), 1)
    told = jnp.zeros((devices, lanes), jnp.float32)
    index = jnp.zeros((devices, lanes), jnp.int32)
    for at in range(levels - 1):
        hits = owner_ids == owner_ref[at : at + 1, :]
        block_row = (block_ref[at : at + 1, :] + 1).astype(jnp.float32)
        first = jnp.min(jnp.where(hits, record_ids, records - 1), axis=1, keepdims=True)
        last = jnp.max(jnp.where(hits, record_ids, 0), axis=1, keepdims=True)
        for copy_at, record in enumerate((first, last)):
            chosen = jnp.where(hits & (record_ids == record), block_row, 0.0)
            label = jnp.sum(chosen, axis=1, keepdims=True)
            told = jnp.where(lane_ids == at * CAP + copy_at, label, told)
            index = jnp.where(lane_ids == at * CAP + copy_at, record, index)
    record_vmem[...] = index
    record_copy = pltpu.make_async_copy(record_vmem, record_ref, small_sem.at[2])
    record_copy.start()
    names_out_ref[...] = told.reshape(devices, 1, lanes)
    names_ref[pl.ds(me, 1)] = names_out_ref[pl.ds(me, 1)]

    right_load.wait()
    spread(0)
    smalls[0].wait()
    smalls[1].wait()
    for copy in first_loads:
        copy.wait()
    for copy in rest_loads:
        copy.start()

    solve(0, 0, None)
    place, message = make(0, 0, record_copy)
    over(devices * pack // TILE, place)
    keep(0, 0, message)
    pl.semaphore_wait(barrier, devices - 1)

    def tell(index):
        other, where = partner(index)
        pltpu.make_async_remote_copy(
            src_ref=names_out_ref.at[pl.ds(other, 1)],
            dst_ref=names_ref.at[pl.ds(me, 1)],
            send_sem=load_sem.at[0],
            recv_sem=name_recv_sem,
            device_id=where,
            device_id_type=MESH,
        ).start()

    over_partners(tell)

    send(0, 0)

    @pl.loop(1, groups)
    def _(group):
        solve(0, group, None)
        deliver(0, group, *make(0, group))

    for at in range(1, levels):
        spread(at)

    name_part = names_ref.at[pl.ds(0, devices - 1)]
    pltpu.make_async_copy(name_part, name_part, name_recv_sem).wait()
    width = devices * pack
    wanted = -(-(levels - 1) * CAP // 8) * 8
    pick = (
        lax.broadcasted_iota(jnp.int32, (wanted, lanes), 0)
        == lax.broadcasted_iota(jnp.int32, (wanted, lanes), 1)
    ).astype(jnp.float32)
    names = lax.dot_general(
        pick,
        names_ref[...].reshape(devices, lanes),
        (((1,), (1,)), ((), ())),
        preferred_element_type=jnp.float32,
    )
    widen = (
        lax.broadcasted_iota(jnp.int32, (devices, width), 0)
        == lax.broadcasted_iota(jnp.int32, (devices, width), 1) // pack
    ).astype(jnp.float32)
    wide = jnp.dot(names, widen, preferred_element_type=jnp.float32).astype(jnp.int32)
    column = lax.broadcasted_iota(jnp.int32, (1, width), 1)
    height = slots * TILE
    row_ids = lax.broadcasted_iota(jnp.int32, (height, width), 0)
    same = row_ids % rows == lax.broadcasted_iota(jnp.int32, (height, width), 1) % rows
    slot_ids = row_ids // TILE

    def build(source):
        at = source * CAP
        label = wide[at : at + 1]
        for c in range(1, CAP):
            label = jnp.where(column % pack // rows == c, wide[at + c : at + c + 1], label)
        for target in range(source + 1, levels):
            hit = same & (slot_ids == label - (target * slots + 1))
            placer_ref[pair_at(source, target)] = hit.astype(jnp.float32).astype(jnp.bfloat16)

    build(0)
    for copy in rest_loads:
        copy.wait()
    name_part = names_out_ref.at[pl.ds(0, devices - 1)]
    pltpu.make_async_copy(name_part, name_part, load_sem.at[0]).wait()
    for at in range(1, levels):
        if at < levels - 1:
            build(at)
        @pl.loop(0, groups)
        def _(group):
            part = arrived_ref.at[at - 1, group, pl.ds(0, (devices - 1) * pack)]
            pltpu.make_async_copy(part, part, recv_sem.at[(at - 1) % 2, group]).wait()
            values = incoming(at - 1, group)
            total = gather(at - 1, at, values)
            for target in range(at + 1, levels):
                work_ref[target, group] = work_ref[target, group] - gather(
                    at - 1, target, values
                )
            solve(at, group, total)
            part = outgoing_ref.at[at - 1, group, pl.ds(0, (devices - 1) * pack)]
            pltpu.make_async_copy(part, part, send_sem.at[group]).wait()
            if at < levels - 1:
                deliver(at, group, *make(at, group))


def shards(
    sizes,
    right_side,
    diag_inverse,
    off_blocks,
    live_counts,
    source_slot,
    target_owner,
    target_block,
):
    levels, slots, rhs, width = right_side.shape
    records = off_blocks.shape[1]
    devices = sizes[0] * sizes[1] * sizes[2]
    lanes = 128
    pack = CAP * rhs // GROUPS
    pairs = levels * (levels - 1) // 2
    vmem = pl.BlockSpec(memory_space=pltpu.VMEM)
    anywhere = pl.BlockSpec(memory_space=pl.ANY)
    messages = (levels - 1, GROUPS, devices * pack, width)
    return pl.pallas_call(
        functools.partial(kernel, sizes),
        out_shape=pltpu.VMEM((levels, slots, rhs, width), jnp.float32),
        in_specs=[anywhere] * 7,
        out_specs=vmem,
        scratch_shapes=[
            pltpu.SMEM((1, levels), jnp.int32),
            pltpu.SMEM(source_slot.shape, jnp.int32),
            pltpu.VMEM(target_owner.shape, jnp.int32),
            pltpu.VMEM(target_block.shape, jnp.int32),
            pltpu.VMEM((levels * slots * rhs, width), jnp.float32),
            pltpu.VMEM((levels, GROUPS, slots * rhs, width), jnp.float32),
            pltpu.VMEM(diag_inverse.shape, diag_inverse.dtype),
            pltpu.VMEM(off_blocks.shape, off_blocks.dtype),
            pltpu.VMEM((slots, rhs, width), jnp.float32),
            pltpu.VMEM((records, rhs, width), jnp.float32),
            pltpu.VMEM(messages, jnp.float32),
            pltpu.VMEM(messages, jnp.float32),
            pltpu.VMEM((pairs, slots * rhs, devices * pack), jnp.bfloat16),
            pltpu.VMEM((devices, 1, lanes), jnp.float32),
            pltpu.VMEM((devices, 1, lanes), jnp.float32),
            pltpu.VMEM((devices, lanes), jnp.int32),
            pltpu.SMEM((devices, lanes), jnp.int32),
            pltpu.SemaphoreType.DMA((4,)),
            pltpu.SemaphoreType.DMA((3,)),
            pltpu.SemaphoreType.DMA((GROUPS,)),
            pltpu.SemaphoreType.DMA((2, GROUPS)),
            pltpu.SemaphoreType.DMA,
        ],
        compiler_params=pltpu.CompilerParams(
            collective_id=0, has_side_effects=True, vmem_limit_bytes=60 * 1024 * 1024
        ),
    )(
        live_counts.reshape(1, levels),
        source_slot,
        target_owner,
        target_block,
        right_side.reshape(levels * slots * rhs, width),
        diag_inverse,
        off_blocks,
    )


def solution(mesh):
    sizes = tuple(mesh.shape[axis] for axis in AXES)
    in_specs = (
        P(None, AXES, None, None),
        P(None, AXES, None, None),
        P(None, AXES, None, None),
        P(None, AXES),
        P(None, AXES),
        P(None, AXES),
        P(None, AXES),
    )
    return jax.shard_map(
        functools.partial(shards, sizes),
        mesh=mesh,
        in_specs=in_specs,
        out_specs=P(None, AXES, None, None),
        check_vma=False,
    )
```
